32 devices in a mesh: rep: 2 (over y), tile: 4 (over z), pen: 2 (over x), sub: 2 (over core).
Axes of the slice: x: 2, y: 2, z: 4, core: 2. Of those that a mesh axis runs over, the one named last changes fastest.
Arguments:
- positions: float32 [6, 4, 2, 512], P('rep', 'tile', 'pen'), parts along dimension 0, may hold values from 0 to 256, as said below
- velocities: float32 [6, 4, 2, 512], P('rep', 'tile', 'pen'), parts along dimension 0, may hold values from -5 to 5
- charges: float32 [8, 2, 512], P(('rep', 'tile'), 'pen'), parts along dimension 0, may hold values from -3 to 3
- inverse_mass: float32 [8, 2, 512], P(('rep', 'tile'), 'pen'), parts along dimension 0, may hold values from 0.06 to 1
- export_rows: int32 [8, 2, 128], P(('rep', 'tile'), 'pen'), parts along dimension 0, may hold values from 0 to 511, as said below
- partners: int32 [8, 2, 64, 512], P(('rep', 'tile'), 'pen', 'sub'), parts along dimension 0, may hold values from 0 to 1663, as said below
- bond_partners: int32 [8, 2, 4, 512], P(('rep', 'tile'), 'pen', 'sub'), parts along dimension 0, may hold values from 0 to 511, as said below
- bond_rest: float32 [8, 2, 4, 512], P(('rep', 'tile'), 'pen', 'sub'), parts along dimension 0, may hold values from 1 to 8
- block_offsets: int32 [6, 4, 2, 512], P('rep', 'tile', 'pen'), parts along dimension 0, may hold values from -1 to 254, as said below
Outputs:
- final_positions: float32 [6, 4, 2, 512], P('rep', 'tile', 'pen'), parts along dimension 0
- final_velocities: float32 [6, 4, 2, 512], P('rep', 'tile', 'pen'), parts along dimension 0
- potential: float32 [8, 2, 512], P(('rep', 'tile'), 'pen', 'sub'), parts along dimension 0
The draws below stay inside these ranges and needn't reach their ends.
There are 2 independent parts, one for each index of `rep`. The reference program is written for one: setup_inputs(seed, part) draws one part's arguments, and reference() takes and returns one part's arrays. A program takes and returns all parts, laid end to end along the dimension named above; each array names one. Nothing has to cross between parts.
Inputs may be any that keep to these rules, and one draw needn't show every extreme that they name: `positions`: coordinates of an atom lie strictly between its block offset + 1 and its block offset + 2, coordinate by coordinate. `block_offsets`: for the patch (t, p), x offsets lie in t * 64 - 1 to t * 64 + 62 and y offsets in p * 128 - 1 to p * 128 + 126; z offsets lie in -1 to 254. `export_rows`: rows of the patch's own atoms. `partners`: columns of the patch's table; columns 1024 to 1151 are never named. Slots that an atom does not use name the atom itself. `bond_partners`: rows of the patch's own atoms.
All inputs are finite; a program needn't handle non-finite values.
Results may differ from the reference program's by a relative error of at most 0.0005.
Values sent between devices are 32-bit elements; how exact they have to be, the bound alone decides.
A program may use at most 128 MiB of HBM per device.

```python
import math
import jax
import jax.numpy as jnp
from jax import lax

GRID = 256
ATOMS = 512
NEIGH = 32
BONDS = 2
INNER = 4
EXPORT = 128
N_TILE = 4
N_PEN = 2


def atom_layout(key):
    keys = jax.random.split(jax.random.fold_in(key, 17), 4)
    shape = (N_TILE, N_PEN, ATOMS)
    planes_x = GRID // N_TILE
    rows_y = GRID // N_PEN
    tiles = jnp.arange(N_TILE, dtype=jnp.int32)[:, None, None]
    pens = jnp.arange(N_PEN, dtype=jnp.int32)[None, :, None]
    atoms = jnp.arange(ATOMS, dtype=jnp.int32)[None, None, :]
    offset_x = tiles * planes_x - 1 + jax.random.randint(keys[0], shape, 0, planes_x)
    offset_y = pens * rows_y - 1 + jax.random.randint(keys[1], shape, 0, rows_y)
    offset_z = jnp.clip(atoms * GRID // ATOMS + jax.random.randint(keys[2], shape, -2, 3), -1, GRID - 2)
    offsets = jnp.stack([offset_x, offset_y, jnp.broadcast_to(offset_z, shape)]).astype(jnp.int32)
    return (offsets, keys[3])


def draw_positions(key, part):
    offsets, frac_key = atom_layout(key)
    frac = jnp.clip(0.5 + 0.18 * jax.random.normal(frac_key, offsets.shape, jnp.float32), 0.05, 0.95)
    return offsets.astype(jnp.float32) + 1.0 + frac


def draw_block_offsets(key, part):
    offsets, frac_key = atom_layout(key)
    return offsets


def draw_export_rows(key, part):
    drawn = jax.random.fold_in(key, 23)
    stride = ATOMS // EXPORT
    rows = jnp.arange(EXPORT, dtype=jnp.int32)[None, None, :] * stride
    return (rows + jax.random.randint(drawn, (N_TILE, N_PEN, EXPORT), 0, stride)).astype(jnp.int32)


def draw_partners(key, part):
    keys = jax.random.split(jax.random.fold_in(key, 29), 5)
    shape = (N_TILE, N_PEN, 2 * NEIGH, ATOMS)
    atoms = jnp.arange(ATOMS, dtype=jnp.int32)[None, None, None, :]
    reach = max(1, 6 * ATOMS // GRID)
    near = jnp.clip(atoms + jax.random.randint(keys[0], shape, -reach, reach + 1), 0, ATOMS - 1)
    neighbour = jax.random.randint(keys[1], shape, 0, 8)
    neighbour = jnp.where(neighbour >= 4, neighbour + 1, neighbour)
    spread = max(1, 6 * EXPORT // GRID)
    column = jnp.clip(atoms * EXPORT // ATOMS + jax.random.randint(keys[2], shape, -spread, spread + 1), 0, EXPORT - 1)
    distant = ATOMS + neighbour * EXPORT + column
    picked = jnp.where(jax.random.randint(keys[3], shape, 0, 2) == 0, near, distant)
    live = jax.random.randint(keys[4], (N_TILE, N_PEN, 1, ATOMS), NEIGH // 2, 2 * NEIGH + 1)
    slots = jnp.arange(2 * NEIGH, dtype=jnp.int32)[None, None, :, None]
    return jnp.where(slots < live, picked, atoms).astype(jnp.int32)


def draw_bond_partners(key, part):
    keys = jax.random.split(jax.random.fold_in(key, 31), 2)
    shape = (N_TILE, N_PEN, 2 * BONDS, ATOMS)
    atoms = jnp.arange(ATOMS, dtype=jnp.int32)[None, None, None, :]
    length = jax.random.randint(keys[0], shape, 1, 4)
    upward = jax.random.randint(keys[1], shape, 0, 2) * 2 - 1
    return jnp.clip(atoms + length * upward, 0, ATOMS - 1).astype(jnp.int32)


def block_levels(stream_key, shape, cuts, smallest, largest):
    def one(dim, parts):
        steps = jax.random.uniform(jax.random.fold_in(jax.random.fold_in(stream_key, 6), dim), (parts,), jnp.float32, smallest / len(cuts), largest / len(cuts))
        return jnp.repeat(jnp.exp(steps), shape[dim] // parts).reshape((-1,) + (1,) * (len(shape) - dim - 1))

    loudness = one(*cuts[0])
    for cut in cuts[1:]:
        loudness = loudness * one(*cut)
    return loudness


def normal_values(stream_key, shape, width, limit, shards=(), kind=jnp.bfloat16):
    factor_of = block_levels(stream_key, shape, shards, -0.22, 0.18) if shards else 1.0
    entries = jax.random.normal(stream_key, shape, jnp.float32) * width * factor_of
    return jnp.minimum(jnp.maximum(entries, -limit), limit).astype(kind)


def setup_inputs(seed: int = 0, part: int = 0) -> dict:
    seeds = jax.random.split(jax.random.key(seed), 10)
    part_keys = jax.random.split(jax.random.fold_in(seeds[9], part), 10)
    return {
        "positions": draw_positions(jax.random.fold_in(jax.random.fold_in(seeds[9], part), 71), part),
        "velocities": normal_values(part_keys[1], (3, N_TILE, N_PEN, ATOMS), 1.0, 5.0, ((1, 4), (2, 2)), jnp.float32),
        "charges": normal_values(part_keys[2], (N_TILE, N_PEN, ATOMS), 0.5, 3.0, ((0, 4), (1, 2)), jnp.float32),
        "inverse_mass": jnp.clip(jnp.exp(math.log(1.0) - 2.8134107 * jax.random.uniform(part_keys[3], (N_TILE, N_PEN, ATOMS), jnp.float32) ** block_levels(part_keys[3], (N_TILE, N_PEN, ATOMS), ((0, 4), (1, 2)), -0.2, 0.2)), 0.06, 1.0),
        "export_rows": draw_export_rows(jax.random.fold_in(jax.random.fold_in(seeds[9], part), 71), part),
        "partners": draw_partners(jax.random.fold_in(jax.random.fold_in(seeds[9], part), 71), part),
        "bond_partners": draw_bond_partners(jax.random.fold_in(jax.random.fold_in(seeds[9], part), 71), part),
        "bond_rest": jnp.clip(1.0 + 7.0 * jax.random.uniform(part_keys[7], (N_TILE, N_PEN, 2 * BONDS, ATOMS), jnp.float32) ** block_levels(part_keys[7], (N_TILE, N_PEN, 2 * BONDS, ATOMS), ((0, 4), (1, 2), (2, 2)), -0.2, 0.2), 1.0, 8.0),
        "block_offsets": draw_block_offsets(jax.random.fold_in(jax.random.fold_in(seeds[9], part), 71), part),
    }


time_step = 0.1
coulomb = 30.0
bond_stiffness = 0.2
soften = 1.0
cutoff_sq = 144.0
ewald_beta = 0.32
highest = lax.Precision.HIGHEST

def spline_pieces(frac):
    rest = 1.0 - frac
    cube = frac * frac * frac
    square = frac * frac
    return (rest * rest * rest / 6.0, (3.0 * cube - 6.0 * square + 4.0) / 6.0, (-3.0 * cube + 3.0 * square + 3.0 * frac + 1.0) / 6.0, cube / 6.0)

def axis_weights(cells, offset, frac, wrapped):
    place = cells[:, None] - offset[None, :]
    if wrapped:
        place = jnp.mod(place, GRID)
    pieces = spline_pieces(frac)
    total = jnp.zeros(place.shape, frac.dtype)
    for order in range(4):
        total = total + jnp.where(place == order, pieces[order][None, :], 0.0)
    return total

def patch_weights(place, offsets, tile_index, pen_index, planes_x, rows_y):
    frac = place - (offsets.astype(place.dtype) + 1.0)
    cells_x = tile_index * planes_x - 1 + jnp.arange(planes_x + 3, dtype=jnp.int32)
    cells_y = pen_index * rows_y - 1 + jnp.arange(rows_y + 3, dtype=jnp.int32)
    weight_x = axis_weights(cells_x, offsets[0], frac[0], False)
    weight_y = axis_weights(cells_y, offsets[1], frac[1], False)
    depth = axis_weights(jnp.arange(GRID, dtype=jnp.int32), offsets[2], frac[2], True)
    plane = (weight_x[:, None, :] * weight_y[None, :, :]).reshape(-1, place.shape[1])
    return (plane, depth)

def influence(freq_x, freq_y, freq_z):

    def signed(freq):
        return jnp.where(freq > GRID // 2, freq - GRID, freq).astype(jnp.float32)

    def modulus(freq):
        angle = 2.0 * math.pi / GRID * freq.astype(jnp.float32)
        real = (1.0 + 4.0 * jnp.cos(angle) + jnp.cos(2.0 * angle)) / 6.0
        imag = (4.0 * jnp.sin(angle) + jnp.sin(2.0 * angle)) / 6.0
        return 1.0 / (real * real + imag * imag)
    sx, sy, sz = (signed(freq_x), signed(freq_y), signed(freq_z))
    m_sq = (sx[:, None, None] ** 2 + sy[None, :, None] ** 2 + sz[None, None, :] ** 2) / float(GRID * GRID)
    anchor = (freq_x[:, None, None] == 0) & (freq_y[None, :, None] == 0) & (freq_z[None, None, :] == 0)
    safe = jnp.where(anchor, 1.0, m_sq)
    value = jnp.exp(-(math.pi / ewald_beta) ** 2 * safe) / (math.pi * float(GRID) ** 3 * safe)
    value = value * modulus(freq_x)[:, None, None] * modulus(freq_y)[None, :, None] * modulus(freq_z)[None, None, :]
    return jnp.where(anchor, 0.0, value)

def hartley(field, axis):
    spectrum = jnp.fft.fft(field, axis=axis)
    return jnp.real(spectrum) - jnp.imag(spectrum)

def pair_force(table, own, charge, neighbours, bonded, rest):
    near = table[:, neighbours]
    delta = own[:, None, :] - near[:3]
    dist_sq = lax.optimization_barrier(jnp.sum(delta * delta, axis=0))
    taper = jnp.where(dist_sq < cutoff_sq, (1.0 - dist_sq / cutoff_sq) ** 2, 0.0)
    strength = coulomb * charge[None, :] * near[3] * taper * (dist_sq + soften) ** (-1.5)
    force = lax.optimization_barrier(jnp.sum(strength[None] * delta, axis=1))
    bond_delta = own[:, None, :] - table[:3][:, bonded]
    length = jnp.sqrt(lax.optimization_barrier(jnp.sum(bond_delta * bond_delta, axis=0)) + soften)
    pull = -bond_stiffness * (length - rest) / length
    return force + lax.optimization_barrier(jnp.sum(pull[None] * bond_delta, axis=1))

def halo_table(coords, charges, export_rows, tiles, pens):
    index = jnp.broadcast_to(export_rows[None], (3,) + export_rows.shape)
    sent = jnp.take_along_axis(coords, index, axis=3)
    sent_charge = jnp.take_along_axis(charges, export_rows, axis=2)
    stacked = jnp.concatenate([sent, sent_charge[None]], axis=0)
    blocks = []
    for across in range(3):
        near_x = tiles + across - 1
        move_x = jnp.where(near_x < 0, -float(GRID), jnp.where(near_x >= N_TILE, float(GRID), 0.0))
        for along in range(3):
            near_y = pens + along - 1
            move_y = jnp.where(near_y < 0, -float(GRID), jnp.where(near_y >= N_PEN, float(GRID), 0.0))
            moved = jnp.roll(stacked, (1 - across, 1 - along), axis=(1, 2))
            blank = jnp.zeros((N_TILE, N_PEN), jnp.float32)
            offset = jnp.stack([jnp.broadcast_to(move_x[:, None], (N_TILE, N_PEN)), jnp.broadcast_to(move_y[None, :], (N_TILE, N_PEN)), blank, blank])
            blocks.append(moved + offset[..., None].astype(moved.dtype))
    own = jnp.concatenate([coords, charges[None]], axis=0)
    return jnp.concatenate([own] + blocks, axis=3)

def reference(positions, velocities, charges, inverse_mass, export_rows, partners, bond_partners, bond_rest, block_offsets):
    planes_x = GRID // N_TILE
    rows_y = GRID // N_PEN
    patch_count = N_TILE * N_PEN
    tiles = jnp.arange(N_TILE, dtype=jnp.int32)
    pens = jnp.arange(N_PEN, dtype=jnp.int32)
    tile_ids = jnp.repeat(tiles, N_PEN)
    pen_ids = jnp.tile(pens, N_TILE)
    flat_partners = partners.reshape(patch_count, -1, ATOMS)
    flat_bonds = bond_partners.reshape(patch_count, -1, ATOMS)
    flat_rest = bond_rest.reshape(patch_count, -1, ATOMS)
    flat_charge = charges.reshape(patch_count, ATOMS)
    coords, speeds = (positions, velocities)

    def patch_force(item):
        table, own, charge, neighbours, bonded, rest = item
        return pair_force(table, own, charge, neighbours, bonded, rest)
    for step in range(INNER):
        table = halo_table(coords, charges, export_rows, tiles, pens)
        flat_table = jnp.transpose(table, (1, 2, 0, 3)).reshape(patch_count, 4, -1)
        flat_coords = jnp.transpose(coords, (1, 2, 0, 3)).reshape(patch_count, 3, ATOMS)
        force = lax.map(patch_force, (flat_table, flat_coords, flat_charge, flat_partners, flat_bonds, flat_rest))
        force = jnp.transpose(force.reshape(N_TILE, N_PEN, 3, ATOMS), (2, 0, 1, 3))
        speeds = speeds + time_step * inverse_mass[None] * force
        coords = coords + time_step * speeds
    flat_coords = jnp.transpose(coords, (1, 2, 0, 3)).reshape(patch_count, 3, ATOMS)
    flat_offsets = jnp.transpose(block_offsets, (1, 2, 0, 3)).reshape(patch_count, 3, ATOMS)

    def spread_patch(item):
        place, offsets, charge, tile_index, pen_index = item
        plane, depth = patch_weights(place, offsets, tile_index, pen_index, planes_x, rows_y)
        local = jnp.einsum('pa,za->pz', plane * charge[None, :], depth, precision=highest)
        return local.reshape(planes_x + 3, rows_y + 3, GRID)
    blocks = lax.map(spread_patch, (flat_coords, flat_offsets, flat_charge, tile_ids, pen_ids))
    blocks = blocks.reshape(N_TILE, N_PEN, planes_x + 3, rows_y + 3, GRID)
    inner_x = blocks[:, :, 1:planes_x + 1]
    from_above = jnp.roll(blocks[:, :, 0:1], -1, axis=0)
    from_below = jnp.roll(blocks[:, :, planes_x + 1:], 1, axis=0)
    inner_x = inner_x.at[:, :, 0:2].add(from_below).at[:, :, planes_x - 1:].add(from_above)
    from_right = jnp.roll(inner_x[:, :, :, 0:1], -1, axis=1)
    from_left = jnp.roll(inner_x[:, :, :, rows_y + 1:], 1, axis=1)
    core = inner_x[:, :, :, 1:rows_y + 1]
    core = core.at[:, :, :, 0:2].add(from_left).at[:, :, :, rows_y - 1:].add(from_right)
    charge_grid = jnp.transpose(core, (0, 2, 1, 3, 4)).reshape(GRID, GRID, GRID)
    spectrum = hartley(hartley(hartley(charge_grid, 2), 1), 0)
    freq = jnp.arange(GRID, dtype=jnp.int32)
    weighted = spectrum * influence(freq, freq, freq)
    potential_grid = hartley(hartley(hartley(weighted, 0), 1), 2)
    padded = jnp.pad(potential_grid, ((1, 2), (1, 2), (0, 0)), mode='wrap')

    def read_patch(item):
        place, offsets, tile_index, pen_index = item
        plane, depth = patch_weights(place, offsets, tile_index, pen_index, planes_x, rows_y)
        corner = (tile_index * planes_x, pen_index * rows_y, jnp.int32(0))
        block = lax.dynamic_slice(padded, corner, (planes_x + 3, rows_y + 3, GRID))
        values = jnp.dot(block.reshape(-1, GRID), depth, precision=highest)
        return lax.optimization_barrier(jnp.sum(values * plane, axis=0))
    potential = lax.map(read_patch, (flat_coords, flat_offsets, tile_ids, pen_ids))
    return (coords, speeds, potential.reshape(N_TILE, N_PEN, ATOMS))
```

```python
import functools
import math

import jax
import jax.numpy as jnp
import numpy as np
from jax import lax
from jax.experimental import pallas as pl
from jax.experimental.pallas import tpu as pltpu
from jax.sharding import PartitionSpec as P

GRID = 256
INNER = 4
LANES = 128

time_step = 0.1
coulomb = 30.0
bond_stiffness = 0.2
soften = 1.0
cutoff_sq = 144.0
ewald_beta = 0.32

f32 = jnp.float32
bf16 = jnp.bfloat16


def lane_gather(rows, low):
    return jnp.take_along_axis(rows, low, axis=1, mode="promise_in_bounds")


def shown_rows(state, shown):
    index = jnp.broadcast_to(shown, (8, shown.shape[1]))
    low, high = index & (LANES - 1), index >> 7
    total = jnp.zeros((8, shown.shape[1]), f32)
    for block in range(state.shape[1] // LANES):
        part = lane_gather(state[:, block * LANES : (block + 1) * LANES], low)
        total = jnp.where(high == block, part, total)
    return total[:4]


def export_kernel(state_ref, shown_ref, sent_ref):
    sent_ref[...] = shown_rows(state_ref[...], shown_ref[...])


def step_kernel(
    place_ref, state_ref, beside_ref, shown_ref, partners_ref, bonds_ref, rest_ref,
    out_ref, sent_ref, table, *, tile_count, pen_count,
):
    atoms = state_ref.shape[1]
    own_blocks = atoms // LANES
    halo_blocks = beside_ref.shape[2] // LANES
    tile_index, pen_index = place_ref[0], place_ref[1]
    blocks = list(range(own_blocks))
    for block in range(own_blocks):
        for row in range(4):
            table[block * 4 + row] = jnp.broadcast_to(
                state_ref[row : row + 1, block * LANES : (block + 1) * LANES], (8, LANES)
            )
    for i in range(3):
        near_x = tile_index + (i - 1)
        move_x = jnp.where(near_x < 0, -float(GRID), jnp.where(near_x >= tile_count, float(GRID), 0.0))
        for j in range(3):
            if i == 1 and j == 1:
                continue
            near_y = pen_index + (j - 1)
            move_y = jnp.where(near_y < 0, -float(GRID), jnp.where(near_y >= pen_count, float(GRID), 0.0))
            patch = beside_ref[j * 3 + i]
            for part in range(halo_blocks):
                block = own_blocks + (i * 3 + j) * halo_blocks + part
                blocks.append(block)
                for row in range(4):
                    line = patch[row : row + 1, part * LANES : (part + 1) * LANES]
                    if row == 0:
                        line = line + move_x
                    if row == 1:
                        line = line + move_y
                    table[block * 4 + row] = jnp.broadcast_to(line, (8, LANES))

    def fetch(index, rows, among):
        low, high = index & (LANES - 1), index >> 7
        found = [jnp.zeros((8, LANES), f32) for _ in range(rows)]
        for block in among:
            hit = high == block
            for row in range(rows):
                found[row] = jnp.where(hit, lane_gather(table[block * 4 + row], low), found[row])
        return found

    for c in range(own_blocks):
        lanes = slice(c * LANES, (c + 1) * LANES)
        own = [jnp.broadcast_to(state_ref[r : r + 1, lanes], (8, LANES)) for r in range(4)]

        def slots(g, force, lanes=lanes, own=own):
            index = partners_ref[pl.ds(pl.multiple_of(g * 8, 8), 8), lanes]
            near = fetch(index, 4, blocks)
            delta = [own[r] - near[r] for r in range(3)]
            dist_sq = delta[0] * delta[0] + delta[1] * delta[1] + delta[2] * delta[2]
            taper = 1.0 - dist_sq / cutoff_sq
            taper = jnp.where(dist_sq < cutoff_sq, taper * taper, 0.0)
            root = lax.rsqrt(dist_sq + soften)
            strength = coulomb * own[3] * near[3] * taper * (root * root * root)
            return tuple(force[r] + strength * delta[r] for r in range(3))

        def bonded(g, force, lanes=lanes, own=own):
            rows = pl.ds(pl.multiple_of(g * 8, 8), 8)
            near = fetch(bonds_ref[rows, lanes], 3, range(own_blocks))
            delta = [own[r] - near[r] for r in range(3)]
            root = lax.rsqrt(delta[0] * delta[0] + delta[1] * delta[1] + delta[2] * delta[2] + soften)
            pull = -bond_stiffness * (1.0 - rest_ref[rows, lanes] * root)
            return tuple(force[r] + pull * delta[r] for r in range(3))

        force = tuple(jnp.zeros((8, LANES), f32) for _ in range(3))
        force = lax.fori_loop(0, partners_ref.shape[0] // 8, slots, force)
        force = lax.fori_loop(0, bonds_ref.shape[0] // 8, bonded, force)
        scale = state_ref[7:8, lanes]
        for r in range(3):
            total = jnp.sum(force[r], axis=0, keepdims=True)
            speed = state_ref[4 + r : 5 + r, lanes] + time_step * scale * total
            out_ref[4 + r : 5 + r, lanes] = speed
            out_ref[r : r + 1, lanes] = state_ref[r : r + 1, lanes] + time_step * speed
        out_ref[3:4, lanes] = state_ref[3:4, lanes]
        out_ref[7:8, lanes] = scale
    sent_ref[...] = shown_rows(out_ref[...], shown_ref[...])


def split(value):
    high = value.astype(bf16)
    return high, (value - high.astype(f32)).astype(bf16)


def product(left, right, turned=False):
    dims = (((1,), (1 if turned else 0,)), ((), ()))

    def dot(a, b):
        return lax.dot_general(a, b, dims, preferred_element_type=f32)

    return dot(left[0], right[0]) + (dot(left[0], right[1]) + dot(left[1], right[0]))


def spline(place, frac):
    rest = 1.0 - frac
    square = frac * frac
    cube = square * frac
    pieces = (
        rest * rest * rest / 6.0,
        (3.0 * cube - 6.0 * square + 4.0) / 6.0,
        (-3.0 * cube + 3.0 * square + 3.0 * frac + 1.0) / 6.0,
        cube / 6.0,
    )
    total = jnp.zeros(place.shape, f32)
    for order in range(4):
        total = jnp.where(place == order, pieces[order], total)
    return total


def mesh_kernel(
    first_ref, lines_ref, squares_ref, atoms_ref, mine_ref, cas_ref, wide_ref, tall_ref, along_ref, across_ref,
    out_ref, grid, wx, wy, wz, *, planes, chunk, keep,
):
    tiles, share, deep = grid.shape[0], grid.shape[1], grid.shape[2]
    atoms = atoms_ref.shape[2]
    first = first_ref[0]

    def cells(offset, count):
        return lax.broadcasted_iota(jnp.int32, (count, atoms), 0) - offset

    def prepare(s):
        own = atoms_ref[s]
        offset = own[3:6].astype(jnp.int32)
        depth = spline(cells(offset[2:3], GRID) & (GRID - 1), own[2:3])
        return product((cas_ref[0], cas_ref[1]), split(depth))

    def tile_of(s):
        apart = first_ref[1] - s
        return jnp.where(apart < 0, apart + tiles, apart)

    def spread(s, carry):
        t = tile_of(s)
        own = atoms_ref[s]
        offset = own[3:6].astype(jnp.int32)
        wx[t] = spline(cells(offset[0:1] - (t * planes - 1), deep), own[0:1])
        rows = spline(cells(offset[1:2], GRID) & (GRID - 1), own[1:2])
        wy[t] = product((mine_ref[0], mine_ref[1]), split(rows))
        depth = prepare(s)
        if keep:
            high, low = split(depth)
            wz[t, 0] = high
            wz[t, 1] = low
        charged = split(depth * own[6:7])
        for c in range(0, share, chunk):
            pieces = [wx[t] * wy[t, k : k + 1, :] for k in range(c, c + chunk)]
            plane = split(jnp.concatenate(pieces, axis=0))
            grid[t, c : c + chunk] = product(plane, charged, True).reshape(chunk, deep, GRID)
        return carry

    lax.fori_loop(0, tiles, spread, 0)

    def transform(k, carry):
        line = grid[:, k].reshape(tiles * deep, GRID)
        spectrum = product((wide_ref[0], wide_ref[1]), split(line))
        m_sq = along_ref[...] + squares_ref[first + k]
        anchor = m_sq == 0.0
        value = across_ref[...] * lines_ref[first + k] / jnp.where(anchor, 1.0, m_sq)
        weighted = spectrum * jnp.where(anchor, 0.0, value)
        back = product((tall_ref[0], tall_ref[1]), split(weighted))
        grid[:, k] = back.reshape(tiles, deep, GRID)
        return carry

    lax.fori_loop(0, share, transform, 0)

    def read(s, carry):
        t = tile_of(s)
        if keep:
            depth = (wz[t, 0], wz[t, 1])
        else:
            depth = split(prepare(s))
        total = jnp.zeros((deep, atoms), f32)
        for c in range(0, share, chunk):
            line = split(grid[t, c : c + chunk].reshape(chunk * deep, GRID))
            values = product(line, depth)
            for k in range(chunk):
                total = total + values[k * deep : (k + 1) * deep] * wy[t, c + k : c + k + 1, :]
        out_ref[s] = jnp.sum(total * wx[t], axis=0, keepdims=True)
        return carry

    lax.fori_loop(0, tiles, read, 0)


def halves(table):
    table = jnp.asarray(table.astype(np.float32))
    return jnp.stack(split(table))


def tables(tiles, planes, deep):
    index = np.arange(GRID)
    angle = 2.0 * math.pi / GRID * np.mod(index[:, None] * index[None, :], GRID)
    cas = np.cos(angle) + np.sin(angle)
    place = np.mod(np.arange(tiles)[:, None] * planes - 1 + np.arange(deep)[None, :], GRID).reshape(-1)
    wide = cas[:, place]
    signed = np.where(index > GRID // 2, index - GRID, index).astype(np.float64)
    turn = 2.0 * math.pi / GRID * index
    real = (1.0 + 4.0 * np.cos(turn) + np.cos(2.0 * turn)) / 6.0
    imag = (4.0 * np.sin(turn) + np.sin(2.0 * turn)) / 6.0
    square = signed**2 / float(GRID * GRID)
    line = np.exp(-((math.pi / ewald_beta) ** 2) * square) / (real * real + imag * imag)
    along = square[:, None] + square[None, :]
    across = line[:, None] * line[None, :] / (math.pi * float(GRID) ** 3)
    return cas, wide, line.astype(np.float32), square.astype(np.float32), along.astype(np.float32), across.astype(np.float32)


def passed_along(value, axis, steps):
    count = lax.axis_size(axis)
    pairs = [(source, (source + steps) % count) for source in range(count)]
    return lax.ppermute(value, axis, pairs)


def on_device(
    positions, velocities, charges, inverse_mass, export_rows, partners, bond_partners, bond_rest, block_offsets,
):
    tile_count = lax.axis_size("tile")
    pen_count = lax.axis_size("pen")
    half_count = lax.axis_size("sub")
    patches = tile_count * pen_count
    tile_index = lax.axis_index("tile")
    pen_index = lax.axis_index("pen")
    atoms = positions.shape[3]
    exported = export_rows.shape[2]
    planes = GRID // tile_count
    place = jnp.stack([tile_index, pen_index]).astype(jnp.int32)
    state = jnp.concatenate(
        [positions[:, 0, 0], charges[0], velocities[:, 0, 0], inverse_mass[0]], axis=0
    )
    shown = export_rows[0]
    neighbours = lax.all_gather(
        jnp.concatenate([partners[0, 0], bond_partners[0, 0]], axis=0), "sub", axis=0
    )
    rest = lax.all_gather(bond_rest[0, 0], "sub", axis=0, tiled=True)
    slots = partners.shape[2]
    near = neighbours[:, :slots].reshape(-1, atoms)
    bonds = neighbours[:, slots:].reshape(-1, atoms)
    fill = -bonds.shape[0] % 8
    self_rows = jnp.broadcast_to(jnp.arange(atoms, dtype=jnp.int32), (fill, atoms))
    bonds = jnp.concatenate([bonds, self_rows], axis=0)
    rest = jnp.concatenate([rest, jnp.ones((fill, atoms), f32)], axis=0)
    vmem = pl.BlockSpec(memory_space=pltpu.VMEM)
    smem = pl.BlockSpec(memory_space=pltpu.SMEM)
    sent_shape = jax.ShapeDtypeStruct((4, exported), f32)
    sent = pl.pallas_call(
        export_kernel, out_shape=sent_shape, in_specs=[vmem, vmem], out_specs=vmem
    )(state, shown)
    columns = (atoms + 9 * exported) // LANES
    step_call = pl.pallas_call(
        functools.partial(step_kernel, tile_count=tile_count, pen_count=pen_count),
        out_shape=(jax.ShapeDtypeStruct(state.shape, f32), sent_shape),
        in_specs=[smem] + [vmem] * 6,
        out_specs=(vmem, vmem),
        scratch_shapes=[pltpu.VMEM((columns * 4, 8, LANES), f32)],
    )
    for step in range(INNER):
        column = jnp.stack([passed_along(sent, "tile", 1), sent, passed_along(sent, "tile", -1)])
        low = passed_along(column, "pen", 1)
        high = low if pen_count == 2 else passed_along(column, "pen", -1)
        beside = jnp.concatenate([low, column, high], axis=0)
        state, sent = step_call(place, state, beside, shown, near, bonds, rest)
    coords, speeds = state[0:3], state[4:7]
    offsets = block_offsets[:, 0, 0].astype(f32)
    packed = jnp.concatenate([coords - (offsets + 1.0), offsets, state[3:4], state[3:4]], axis=0)
    row = jnp.concatenate(
        [packed] + [passed_along(packed, "pen", step) for step in range(1, pen_count)], axis=1
    )
    every = jnp.stack([row] + [passed_along(row, "tile", step) for step in range(1, tile_count)])
    share = GRID // (patches * half_count)
    chunk = math.gcd(share, 8)
    unit = 8 if chunk % 2 == 0 else 16
    deep = -(-(planes + 3) // unit) * unit
    wide_atoms = pen_count * atoms
    keep = patches * atoms * GRID * 4 <= 8 * 1024 * 1024
    cas, wide, line, square, along, across = tables(tile_count, planes, deep)
    start = (lax.axis_index(("tile", "pen", "sub")) * share).astype(jnp.int32)
    first = jnp.stack([start, tile_index.astype(jnp.int32)])
    partial_value = pl.pallas_call(
        functools.partial(mesh_kernel, planes=planes, chunk=chunk, keep=keep),
        out_shape=jax.ShapeDtypeStruct((tile_count, 1, wide_atoms), f32),
        in_specs=[smem] * 3 + [vmem] * 7,
        out_specs=vmem,
        scratch_shapes=[
            pltpu.VMEM((tile_count, share, deep, GRID), f32),
            pltpu.VMEM((tile_count, deep, wide_atoms), f32),
            pltpu.VMEM((tile_count, share, wide_atoms), f32),
            pltpu.VMEM((tile_count if keep else 1, 2, GRID, wide_atoms), bf16),
        ],
        compiler_params=pltpu.CompilerParams(vmem_limit_bytes=60 * 1024 * 1024),
    )(
        first, jnp.asarray(line), jnp.asarray(square), every,
        lax.dynamic_slice_in_dim(halves(cas), start, share, axis=1), halves(cas), halves(wide), halves(wide.T), jnp.asarray(along), jnp.asarray(across),
    )
    sums = partial_value[0]
    for step in range(1, tile_count):
        sums = sums + passed_along(partial_value[step], "tile", -step)
    own = sums[:, :atoms]
    for step in range(1, pen_count):
        own = own + passed_along(sums[:, step * atoms : (step + 1) * atoms], "pen", -step)
    half = lax.axis_index("sub")
    width = atoms // half_count
    potential = lax.dynamic_slice_in_dim(own, half * width, width, 1)
    for step in range(1, half_count):
        other = (half + step) % half_count
        potential = potential + passed_along(
            lax.dynamic_slice_in_dim(own, other * width, width, 1), "sub", step
        )
    potential = potential.reshape(-1)
    return (coords[:, None, None, :], speeds[:, None, None, :], potential[None, None, :])


def solution(mesh):
    placed = (
        P("rep", "tile", "pen", None),
        P("rep", "tile", "pen", None),
        P(("rep", "tile"), "pen", None),
        P(("rep", "tile"), "pen", None),
        P(("rep", "tile"), "pen", None),
        P(("rep", "tile"), "pen", "sub", None),
        P(("rep", "tile"), "pen", "sub", None),
        P(("rep", "tile"), "pen", "sub", None),
        P("rep", "tile", "pen", None),
    )
    return jax.shard_map(
        on_device,
        mesh=mesh,
        in_specs=placed,
        out_specs=(
            P("rep", "tile", "pen", None),
            P("rep", "tile", "pen", None),
            P(("rep", "tile"), "pen", "sub"),
        ),
        check_vma=False,
    )
```

```python
import functools
import math

import jax
import jax.numpy as jnp
import numpy as np
from jax import lax
from jax.experimental import pallas as pl
from jax.experimental.pallas import tpu as pltpu
from jax.sharding import PartitionSpec as P

GRID = 256
INNER = 4
LANES = 128

time_step = 0.1
coulomb = 30.0
bond_stiffness = 0.2
soften = 1.0
cutoff_sq = 144.0
ewald_beta = 0.32

f32 = jnp.float32
bf16 = jnp.bfloat16


def lane_gather(rows, low):
    return jnp.take_along_axis(rows, low, axis=1, mode="promise_in_bounds")


def shown_rows(state, shown):
    index = jnp.broadcast_to(shown, (8, shown.shape[1]))
    low, high = index & (LANES - 1), index >> 7
    total = jnp.zeros((8, shown.shape[1]), f32)
    for block in range(state.shape[1] // LANES):
        part = lane_gather(state[:, block * LANES : (block + 1) * LANES], low)
        total = jnp.where(high == block, part, total)
    return total[:4]


def dynamics_kernel(
    state_ref, shown_ref, partners_ref, bonds_ref, rest_ref,
    out_ref, table, sent, beside, send_sem, recv_sem, *, tile_count, pen_count,
):
    tile_index, pen_index = lax.axis_index("tile"), lax.axis_index("pen")
    around = [(i, j) for i in range(3) for j in range(3) if (i, j) != (1, 1)]

    def neighbour(i, j):
        return {
            "tile": lax.rem(tile_index + (i - 1) + tile_count, tile_count),
            "pen": lax.rem(pen_index + (j - 1) + pen_count, pen_count),
        }

    barrier = pltpu.get_barrier_semaphore()
    for i, j in around:
        pl.semaphore_signal(
            barrier, inc=1, device_id=neighbour(i, j), device_id_type=pl.DeviceIdType.MESH
        )
    pl.semaphore_wait(barrier, len(around))
    out_ref[...] = state_ref[...]

    def step(n, carry):
        sent[n] = shown_rows(out_ref[...], shown_ref[...])
        copies = []
        for place, (i, j) in enumerate(around):
            copy = pltpu.make_async_remote_copy(
                src_ref=sent.at[n],
                dst_ref=beside.at[n, len(around) - 1 - place],
                send_sem=send_sem.at[n, place],
                recv_sem=recv_sem.at[n, len(around) - 1 - place],
                device_id=neighbour(i, j),
                device_id_type=pl.DeviceIdType.MESH,
            )
            copy.start()
            copies.append(copy)
        one_step(
            tile_index, pen_index, tile_count, pen_count, n, copies, around,
            out_ref, beside, partners_ref, bonds_ref, rest_ref, table,
        )
        return carry

    lax.fori_loop(0, INNER, step, 0)


def one_step(
    tile_index, pen_index, tile_count, pen_count, n, copies, around,
    state_ref, beside_ref, partners_ref, bonds_ref, rest_ref, table,
):
    out_ref = state_ref
    atoms = state_ref.shape[1]
    own_blocks = atoms // LANES
    halo_blocks = beside_ref.shape[3] // LANES
    blocks = list(range(own_blocks))
    for block in range(own_blocks):
        for row in range(4):
            table[block * 4 + row] = jnp.broadcast_to(
                state_ref[row : row + 1, block * LANES : (block + 1) * LANES], (8, LANES)
            )
    for copy in copies:
        copy.wait()
    for i in range(3):
        near_x = tile_index + (i - 1)
        move_x = jnp.where(near_x < 0, -float(GRID), jnp.where(near_x >= tile_count, float(GRID), 0.0))
        for j in range(3):
            if i == 1 and j == 1:
                continue
            near_y = pen_index + (j - 1)
            move_y = jnp.where(near_y < 0, -float(GRID), jnp.where(near_y >= pen_count, float(GRID), 0.0))
            patch = beside_ref[n, around.index((i, j))]
            for part in range(halo_blocks):
                block = own_blocks + (i * 3 + j) * halo_blocks + part
                blocks.append(block)
                for row in range(4):
                    line = patch[row : row + 1, part * LANES : (part + 1) * LANES]
                    if row == 0:
                        line = line + move_x
                    if row == 1:
                        line = line + move_y
                    table[block * 4 + row] = jnp.broadcast_to(line, (8, LANES))

    def fetch(index, rows, among):
        low, high = index & (LANES - 1), index >> 7
        found = [jnp.zeros((8, LANES), f32) for _ in range(rows)]
        for block in among:
            hit = high == block
            for row in range(rows):
                found[row] = jnp.where(hit, lane_gather(table[block * 4 + row], low), found[row])
        return found

    for c in range(own_blocks):
        lanes = slice(c * LANES, (c + 1) * LANES)
        own = [jnp.broadcast_to(state_ref[r : r + 1, lanes], (8, LANES)) for r in range(4)]

        def slots(g, force, lanes=lanes, own=own):
            index = partners_ref[pl.ds(pl.multiple_of(g * 8, 8), 8), lanes]
            near = fetch(index, 4, blocks)
            delta = [own[r] - near[r] for r in range(3)]
            dist_sq = delta[0] * delta[0] + delta[1] * delta[1] + delta[2] * delta[2]
            taper = 1.0 - dist_sq / cutoff_sq
            taper = jnp.where(dist_sq < cutoff_sq, taper * taper, 0.0)
            root = lax.rsqrt(dist_sq + soften)
            strength = coulomb * own[3] * near[3] * taper * (root * root * root)
            return tuple(force[r] + strength * delta[r] for r in range(3))

        def bonded(g, force, lanes=lanes, own=own):
            rows = pl.ds(pl.multiple_of(g * 8, 8), 8)
            near = fetch(bonds_ref[rows, lanes], 3, range(own_blocks))
            delta = [own[r] - near[r] for r in range(3)]
            root = lax.rsqrt(delta[0] * delta[0] + delta[1] * delta[1] + delta[2] * delta[2] + soften)
            pull = -bond_stiffness * (1.0 - rest_ref[rows, lanes] * root)
            return tuple(force[r] + pull * delta[r] for r in range(3))

        force = tuple(jnp.zeros((8, LANES), f32) for _ in range(3))
        force = lax.fori_loop(0, partners_ref.shape[0] // 8, slots, force)
        force = lax.fori_loop(0, bonds_ref.shape[0] // 8, bonded, force)
        scale = state_ref[7:8, lanes]
        for r in range(3):
            total = jnp.sum(force[r], axis=0, keepdims=True)
            speed = state_ref[4 + r : 5 + r, lanes] + time_step * scale * total
            out_ref[4 + r : 5 + r, lanes] = speed
            out_ref[r : r + 1, lanes] = state_ref[r : r + 1, lanes] + time_step * speed
        out_ref[3:4, lanes] = state_ref[3:4, lanes]
        out_ref[7:8, lanes] = scale


def split(value):
    high = value.astype(bf16)
    return high, (value - high.astype(f32)).astype(bf16)


def product(left, right, turned=False):
    dims = (((1,), (1 if turned else 0,)), ((), ()))

    def dot(a, b):
        return lax.dot_general(a, b, dims, preferred_element_type=f32)

    return dot(left[0], right[0]) + (dot(left[0], right[1]) + dot(left[1], right[0]))


def spline(place, frac):
    rest = 1.0 - frac
    square = frac * frac
    cube = square * frac
    pieces = (
        rest * rest * rest / 6.0,
        (3.0 * cube - 6.0 * square + 4.0) / 6.0,
        (-3.0 * cube + 3.0 * square + 3.0 * frac + 1.0) / 6.0,
        cube / 6.0,
    )
    total = jnp.zeros(place.shape, f32)
    for order in range(4):
        total = jnp.where(place == order, pieces[order], total)
    return total


def mesh_kernel(
    first_ref, lines_ref, squares_ref, atoms_ref, mine_ref, cas_ref, wide_ref, tall_ref, along_ref, across_ref,
    out_ref, grid, wx, wy, wz, *, planes, chunk, keep,
):
    tiles, share, deep = grid.shape[0], grid.shape[1], grid.shape[2]
    atoms = atoms_ref.shape[2]
    first = first_ref[0]

    def cells(offset, count):
        return lax.broadcasted_iota(jnp.int32, (count, atoms), 0) - offset

    def prepare(s):
        own = atoms_ref[s]
        offset = own[3:6].astype(jnp.int32)
        depth = spline(cells(offset[2:3], GRID) & (GRID - 1), own[2:3])
        return product((cas_ref[0], cas_ref[1]), split(depth))

    def tile_of(s):
        apart = first_ref[1] - s
        return jnp.where(apart < 0, apart + tiles, apart)

    def spread(s, carry):
        t = tile_of(s)
        own = atoms_ref[s]
        offset = own[3:6].astype(jnp.int32)
        wx[t] = spline(cells(offset[0:1] - (t * planes - 1), deep), own[0:1])
        rows = spline(cells(offset[1:2], GRID) & (GRID - 1), own[1:2])
        wy[t] = product((mine_ref[0], mine_ref[1]), split(rows))
        depth = prepare(s)
        if keep:
            high, low = split(depth)
            wz[t, 0] = high
            wz[t, 1] = low
        charged = split(depth * own[6:7])
        for c in range(0, share, chunk):
            pieces = [wx[t] * wy[t, k : k + 1, :] for k in range(c, c + chunk)]
            plane = split(jnp.concatenate(pieces, axis=0))
            grid[t, c : c + chunk] = product(plane, charged, True).reshape(chunk, deep, GRID)
        return carry

    lax.fori_loop(0, tiles, spread, 0)

    def transform(k, carry):
        line = grid[:, k].reshape(tiles * deep, GRID)
        spectrum = product((wide_ref[0], wide_ref[1]), split(line))
        m_sq = along_ref[...] + squares_ref[first + k]
        anchor = m_sq == 0.0
        value = across_ref[...] * lines_ref[first + k] / jnp.where(anchor, 1.0, m_sq)
        weighted = spectrum * jnp.where(anchor, 0.0, value)
        back = product((tall_ref[0], tall_ref[1]), split(weighted))
        grid[:, k] = back.reshape(tiles, deep, GRID)
        return carry

    lax.fori_loop(0, share, transform, 0)

    def read(s, carry):
        t = tile_of(s)
        if keep:
            depth = (wz[t, 0], wz[t, 1])
        else:
            depth = split(prepare(s))
        total = jnp.zeros((deep, atoms), f32)
        for c in range(0, share, chunk):
            line = split(grid[t, c : c + chunk].reshape(chunk * deep, GRID))
            values = product(line, depth)
            for k in range(chunk):
                total = total + values[k * deep : (k + 1) * deep] * wy[t, c + k : c + k + 1, :]
        out_ref[s] = jnp.sum(total * wx[t], axis=0, keepdims=True)
        return carry

    lax.fori_loop(0, tiles, read, 0)


def halves(table):
    table = jnp.asarray(table.astype(np.float32))
    return jnp.stack(split(table))


def tables(tiles, planes, deep):
    index = np.arange(GRID)
    angle = 2.0 * math.pi / GRID * np.mod(index[:, None] * index[None, :], GRID)
    cas = np.cos(angle) + np.sin(angle)
    place = np.mod(np.arange(tiles)[:, None] * planes - 1 + np.arange(deep)[None, :], GRID).reshape(-1)
    wide = cas[:, place]
    signed = np.where(index > GRID // 2, index - GRID, index).astype(np.float64)
    turn = 2.0 * math.pi / GRID * index
    real = (1.0 + 4.0 * np.cos(turn) + np.cos(2.0 * turn)) / 6.0
    imag = (4.0 * np.sin(turn) + np.sin(2.0 * turn)) / 6.0
    square = signed**2 / float(GRID * GRID)
    line = np.exp(-((math.pi / ewald_beta) ** 2) * square) / (real * real + imag * imag)
    along = square[:, None] + square[None, :]
    across = line[:, None] * line[None, :] / (math.pi * float(GRID) ** 3)
    return cas, wide, line.astype(np.float32), square.astype(np.float32), along.astype(np.float32), across.astype(np.float32)


def passed_along(value, axis, steps):
    count = lax.axis_size(axis)
    pairs = [(source, (source + steps) % count) for source in range(count)]
    return lax.ppermute(value, axis, pairs)


def on_device(
    positions, velocities, charges, inverse_mass, export_rows, partners, bond_partners, bond_rest, block_offsets,
):
    tile_count = lax.axis_size("tile")
    pen_count = lax.axis_size("pen")
    half_count = lax.axis_size("sub")
    patches = tile_count * pen_count
    tile_index = lax.axis_index("tile")
    pen_index = lax.axis_index("pen")
    atoms = positions.shape[3]
    exported = export_rows.shape[2]
    planes = GRID // tile_count
    state = jnp.concatenate(
        [positions[:, 0, 0], charges[0], velocities[:, 0, 0], inverse_mass[0]], axis=0
    )
    shown = export_rows[0]
    neighbours = lax.all_gather(
        jnp.concatenate([partners[0, 0], bond_partners[0, 0]], axis=0), "sub", axis=0
    )
    rest = lax.all_gather(bond_rest[0, 0], "sub", axis=0, tiled=True)
    slots = partners.shape[2]
    near = neighbours[:, :slots].reshape(-1, atoms)
    bonds = neighbours[:, slots:].reshape(-1, atoms)
    fill = -bonds.shape[0] % 8
    self_rows = jnp.broadcast_to(jnp.arange(atoms, dtype=jnp.int32), (fill, atoms))
    bonds = jnp.concatenate([bonds, self_rows], axis=0)
    rest = jnp.concatenate([rest, jnp.ones((fill, atoms), f32)], axis=0)
    vmem = pl.BlockSpec(memory_space=pltpu.VMEM)
    smem = pl.BlockSpec(memory_space=pltpu.SMEM)
    columns = (atoms + 9 * exported) // LANES
    state = pl.pallas_call(
        functools.partial(dynamics_kernel, tile_count=tile_count, pen_count=pen_count),
        out_shape=jax.ShapeDtypeStruct(state.shape, f32),
        in_specs=[vmem] * 5,
        out_specs=vmem,
        scratch_shapes=[
            pltpu.VMEM((columns * 4, 8, LANES), f32),
            pltpu.VMEM((INNER, 4, exported), f32),
            pltpu.VMEM((INNER, 8, 4, exported), f32),
            pltpu.SemaphoreType.DMA((INNER, 8)),
            pltpu.SemaphoreType.DMA((INNER, 8)),
        ],
        compiler_params=pltpu.CompilerParams(collective_id=0, has_side_effects=True),
    )(state, shown, near, bonds, rest)
    coords, speeds = state[0:3], state[4:7]
    offsets = block_offsets[:, 0, 0].astype(f32)
    packed = jnp.concatenate([coords - (offsets + 1.0), offsets, state[3:4], state[3:4]], axis=0)
    row = jnp.concatenate(
        [packed] + [passed_along(packed, "pen", step) for step in range(1, pen_count)], axis=1
    )
    every = jnp.stack([row] + [passed_along(row, "tile", step) for step in range(1, tile_count)])
    share = GRID // (patches * half_count)
    chunk = math.gcd(share, 8)
    unit = 8 if chunk % 2 == 0 else 16
    deep = -(-(planes + 3) // unit) * unit
    wide_atoms = pen_count * atoms
    keep = patches * atoms * GRID * 4 <= 8 * 1024 * 1024
    cas, wide, line, square, along, across = tables(tile_count, planes, deep)
    start = (lax.axis_index(("tile", "pen", "sub")) * share).astype(jnp.int32)
    first = jnp.stack([start, tile_index.astype(jnp.int32)])
    partial_value = pl.pallas_call(
        functools.partial(mesh_kernel, planes=planes, chunk=chunk, keep=keep),
        out_shape=jax.ShapeDtypeStruct((tile_count, 1, wide_atoms), f32),
        in_specs=[smem] * 3 + [vmem] * 7,
        out_specs=vmem,
        scratch_shapes=[
            pltpu.VMEM((tile_count, share, deep, GRID), f32),
            pltpu.VMEM((tile_count, deep, wide_atoms), f32),
            pltpu.VMEM((tile_count, share, wide_atoms), f32),
            pltpu.VMEM((tile_count if keep else 1, 2, GRID, wide_atoms), bf16),
        ],
        compiler_params=pltpu.CompilerParams(vmem_limit_bytes=60 * 1024 * 1024),
    )(
        first, jnp.asarray(line), jnp.asarray(square), every,
        lax.dynamic_slice_in_dim(halves(cas), start, share, axis=1), halves(cas), halves(wide), halves(wide.T), jnp.asarray(along), jnp.asarray(across),
    )
    sums = partial_value[0]
    for step in range(1, tile_count):
        sums = sums + passed_along(partial_value[step], "tile", -step)
    own = sums[:, :atoms]
    for step in range(1, pen_count):
        own = own + passed_along(sums[:, step * atoms : (step + 1) * atoms], "pen", -step)
    half = lax.axis_index("sub")
    width = atoms // half_count
    potential = lax.dynamic_slice_in_dim(own, half * width, width, 1)
    for step in range(1, half_count):
        other = (half + step) % half_count
        potential = potential + passed_along(
            lax.dynamic_slice_in_dim(own, other * width, width, 1), "sub", step
        )
    potential = potential.reshape(-1)
    return (coords[:, None, None, :], speeds[:, None, None, :], potential[None, None, :])


def solution(mesh):
    placed = (
        P("rep", "tile", "pen", None),
        P("rep", "tile", "pen", None),
        P(("rep", "tile"), "pen", None),
        P(("rep", "tile"), "pen", None),
        P(("rep", "tile"), "pen", None),
        P(("rep", "tile"), "pen", "sub", None),
        P(("rep", "tile"), "pen", "sub", None),
        P(("rep", "tile"), "pen", "sub", None),
        P("rep", "tile", "pen", None),
    )
    return jax.shard_map(
        on_device,
        mesh=mesh,
        in_specs=placed,
        out_specs=(
            P("rep", "tile", "pen", None),
            P("rep", "tile", "pen", None),
            P(("rep", "tile"), "pen", "sub"),
        ),
        check_vma=False,
    )
```
